256 devices in a mesh: gx: 4 (over x), gy: 4 (over z_hi), gz: 16 (over z_lo, y, core).
Axes of the slice: x: 4, y: 4, z: 8 (z_hi: 4, z_lo: 2; z = z_hi * 2 + z_lo), core: 2. Of those that a mesh axis runs over, the one named last changes fastest.
Arguments:
- columns: int32 [8192, 2048], P(('gx', 'gy', 'gz')), may hold values from 0 to 32767, as said below
- counts: int32 [8192, 2048], P(('gx', 'gy', 'gz')), may hold values from 1 to 63
- nnz_count: int32 [8192], P(('gx', 'gy', 'gz')), may hold values from 1 to 2048, as said below
- selected: int32 [2048], replicated, may hold values from 0 to 32767, as said below
Outputs:
- gene_stats: float32 [2, 32768], P(None, 'gz')
- pca_input: bfloat16 [8192, 2048], P(('gx', 'gy'), 'gz')
The draws below stay inside these ranges and needn't reach their ends.
Inputs may be any that keep to these rules, and one draw needn't show every extreme that they name: `columns`: in each row no two slots fall in the same block of 16 consecutive genes (so the first nnz_count slots hold distinct genes); slots beyond nnz_count are not part of the matrix. For every k, the live slots of one cell fall on at most 16 of the genes selected[k * 2048 / 16] to selected[(k + 1) * 2048 / 16 - 1]; some cell reaches 16 for every k in every draw. `nnz_count`: some cell has all 2048 slots live in every draw. `selected`: distinct genes.
All inputs are finite; a program needn't handle non-finite values.
Results may differ from the reference program's by a relative error of at most 0.0085.
Values may be sent and summed in bfloat16 or wider, within the bound.
A program may use at most 128 MiB of HBM per device.

```python
import jax
import jax.numpy as jnp
from jax import lax

GENES = 32768
SEL = 2048
NNZ_MAX = 2048
CELLS = 8192
N_GZ = 16


def block_plan(key):
    stride = GENES // NNZ_MAX
    share_size = SEL // N_GZ
    per_owner = 2 * share_size // stride
    block_order = jax.random.permutation(jax.random.fold_in(key, 31), jnp.arange(NNZ_MAX, dtype=jnp.int32))[:N_GZ * per_owner]
    block_order = block_order.reshape(N_GZ, per_owner).astype(jnp.int32)
    block_keys = jax.random.split(jax.random.fold_in(key, 32), N_GZ * per_owner)
    lane_perm = jax.vmap(lambda one_key: jax.random.permutation(one_key, jnp.arange(stride, dtype=jnp.int32)))(block_keys)
    return (block_order, lane_perm.reshape(N_GZ, per_owner, stride).astype(jnp.int32))


def full_cell(key):
    return jax.random.randint(jax.random.fold_in(key, 41), (), 0, CELLS, dtype=jnp.int32)


def draw_columns(key, part):
    stride = GENES // NNZ_MAX
    block_order, lane_perm = block_plan(key)
    forced = jnp.full((NNZ_MAX,), -1, jnp.int32).at[block_order.reshape(-1)].set(lane_perm[:, :, 0].reshape(-1))
    jitter = jax.random.randint(jax.random.fold_in(key, 12), (CELLS, NNZ_MAX), 0, stride, dtype=jnp.int32)
    cell_ids = lax.broadcasted_iota(jnp.int32, (CELLS, NNZ_MAX), 0)
    pinned = (cell_ids == full_cell(key)) & (forced[None, :] >= 0)
    jitter = jnp.where(pinned, forced[None, :], jitter)
    block_ids = lax.broadcasted_iota(jnp.int32, (CELLS, NNZ_MAX), 1)
    genes_drawn = block_ids * stride + jitter
    shuffled = jax.random.permutation(jax.random.fold_in(key, 14), genes_drawn, axis=1, independent=True)
    return shuffled.astype(jnp.int32)


def draw_nnz_count(key, part):
    cell_ids = jnp.arange(CELLS, dtype=jnp.int32)
    lowest = NNZ_MAX // 3
    base = lowest + (NNZ_MAX - lowest) * cell_ids // max(CELLS - 1, 1)
    floor_count = jnp.maximum(base // 2, 1)
    spread = base - floor_count + 1
    draw_bits = jax.random.randint(jax.random.fold_in(key, 21), (CELLS,), 0, 1 << 20, dtype=jnp.int32)
    picked = floor_count + draw_bits * spread // (1 << 20)
    picked = jnp.where(cell_ids == full_cell(key), NNZ_MAX, picked)
    return jnp.clip(picked, 1, NNZ_MAX).astype(jnp.int32)


def draw_selected(key, part):
    stride = GENES // NNZ_MAX
    share_size = SEL // N_GZ
    per_owner = 2 * share_size // stride
    block_order, lane_perm = block_plan(key)
    gene_grid = block_order[:, :, None] * stride + lane_perm
    anchors = gene_grid[:, :, 0]
    others = gene_grid[:, :, 1:].reshape(N_GZ, per_owner * (stride - 1))
    other_keys = jax.random.split(jax.random.fold_in(key, 33), N_GZ)
    others = jax.vmap(lambda one_key, row_genes: jax.random.permutation(one_key, row_genes))(other_keys, others)
    others = others[:, :share_size - per_owner]
    chosen = jnp.concatenate([anchors, others], axis=1)
    order_keys = jax.random.split(jax.random.fold_in(key, 34), N_GZ)
    chosen = jax.vmap(lambda one_key, row_genes: jax.random.permutation(one_key, row_genes))(order_keys, chosen)
    return chosen.reshape(-1).astype(jnp.int32)


def with_ends(drawn, key, low, top_value):
    longest = drawn.shape.index(max(drawn.shape))
    spots = []
    for shift in (0, 1):
        where = [jax.random.randint(jax.random.fold_in(key, axis), (), 0, length) for axis, length in enumerate(drawn.shape)]
        where[longest] = (where[longest] + shift) % drawn.shape[longest]
        spots.append(tuple(where))
    return drawn.at[spots[0]].set(low).at[spots[1]].set(top_value)


def setup_inputs(seed: int = 0) -> dict:
    streams_of = jax.random.split(jax.random.key(seed), 5)
    return {
        "columns": draw_columns(jax.random.fold_in(streams_of[4], 71), 0),
        "counts": with_ends(jax.random.randint(streams_of[1], (CELLS, NNZ_MAX), 1, 64), jax.random.fold_in(streams_of[1], 1), 1, 63).astype(jnp.int32),
        "nnz_count": draw_nnz_count(jax.random.fold_in(streams_of[4], 71), 0),
        "selected": draw_selected(jax.random.fold_in(streams_of[4], 71), 0),
    }


target_sum = 10000.0
var_floor = 0.01
clip_value = 10.0

def reference(columns, counts, nnz_count, selected):
    slot = lax.broadcasted_iota(jnp.int32, counts.shape, 1)
    live = slot < nnz_count[:, None]
    raw = jnp.where(live, counts.astype(jnp.float32), jnp.float32(0.0))
    library = lax.optimization_barrier(jnp.sum(raw, axis=1, keepdims=True))
    values = jnp.log1p(raw * (target_sum / library))
    genes = jnp.where(live, columns, 0).astype(jnp.int32).reshape(-1)
    flat = values.reshape(-1)
    total = jax.ops.segment_sum(flat, genes, num_segments=GENES)
    square = jax.ops.segment_sum(flat * flat, genes, num_segments=GENES)
    mean = total / CELLS
    variance = square / CELLS - mean * mean
    gene_stats = jnp.stack([mean, variance])
    table = jnp.full((GENES,), SEL, jnp.int32).at[selected].set(jnp.arange(SEL, dtype=jnp.int32))
    position = table[genes]
    rows = jnp.repeat(jnp.arange(CELLS, dtype=jnp.int32), NNZ_MAX)
    index = rows * (SEL + 1) + position
    dense = jax.ops.segment_sum(flat, index, num_segments=CELLS * (SEL + 1)).reshape(CELLS, SEL + 1)[:, :SEL]
    mean_sel = mean[selected]
    scale_sel = jnp.sqrt(jnp.maximum(variance[selected], var_floor))
    pca_input = jnp.clip((dense - mean_sel[None, :]) / scale_sel[None, :], -clip_value, clip_value).astype(jnp.bfloat16)
    return (gene_stats, pca_input)
```

```python
import jax
import jax.numpy as jnp
from jax import lax
from jax.experimental import pallas as pl
from jax.experimental.pallas import tpu as pltpu
from jax.sharding import PartitionSpec as P

target_sum = 10000.0
var_floor = 0.01
clip_value = 10.0
MESH = pl.DeviceIdType.MESH
f32, bf16, i32 = jnp.float32, jnp.bfloat16, jnp.int32


def iota(shape, dim):
    return lax.broadcasted_iota(i32, shape, dim)


def vreg_stage(x, j, p):
    n = x.shape[0]
    if p is None:
        y = x.reshape(n >> (j + 1), 2, 1 << j, 8, 128)
        a, b = y[:, 0], y[:, 1]
        out = jnp.stack([jnp.minimum(a, b), jnp.maximum(a, b)], axis=1)
    else:
        y = x.reshape(n >> (p + 1), 2, 1 << (p - j - 1), 2, 1 << j, 8, 128)
        a, b = y[:, :, :, 0], y[:, :, :, 1]
        lo, hi = jnp.minimum(a, b), jnp.maximum(a, b)
        first = jnp.stack([lo[:, 0], hi[:, 1]], axis=1)
        second = jnp.stack([hi[:, 0], lo[:, 1]], axis=1)
        out = jnp.stack([first, second], axis=3)
    return out.reshape(n, 8, 128)


def sublane_stage(x, d):
    rows = iota(x.shape, 1)
    other = jnp.take_along_axis(x, rows ^ d, axis=1, mode="promise_in_bounds")
    return jnp.where((rows & d) == 0, jnp.minimum(x, other), jnp.maximum(x, other))


def lane_stage(x, d):
    flat = x.reshape(x.shape[0] * 8, 128)
    lanes = iota(flat.shape, 1)
    other = jnp.take_along_axis(flat, lanes ^ d, axis=1, mode="promise_in_bounds")
    out = jnp.where((lanes & d) == 0, jnp.minimum(flat, other), jnp.maximum(flat, other))
    return out.reshape(x.shape)


def sort_words(x):
    place = iota((1, 8, 128), 1) * 64 + (iota((1, 8, 128), 2) >> 5) * 512

    def sign(p):
        return jnp.where(((place >> p) & 1) == 0, f32(1.0), f32(-1.0))

    held = None
    for p in range(1, 12):
        if p >= 6:
            change = sign(p) if p < 11 else None
            if held is not None:
                change = held if change is None else change * held
            x = x * change
            held = sign(p)
        for j in reversed(range(p)):
            if j >= 9:
                x = lane_stage(x, 32 << (j - 9))
            elif j >= 6:
                x = sublane_stage(x, 1 << (j - 6))
            else:
                x = vreg_stage(x, j, p if p < 6 else None)
    return x


def make_words(columns, raw):
    place = ((columns << 6) & ((0x600 << 10) | (15 << 6))) | ((columns << 12) & (7 << 16))
    return place | ((columns << 3) & (63 << 10)) | raw


def sort_rows(tiles):
    x = jnp.concatenate(
        [jnp.concatenate(tiles[4 * m : 4 * m + 4], axis=0).T for m in range(4)], axis=0
    )
    x = sort_words(x.reshape(64, 8, 128)).reshape(4, 128, 128)
    turned = [x[m].T for m in range(4)]
    return [turned[owner % 4][32 * (owner // 4) : 32 * (owner // 4) + 32] for owner in range(16)]


def kernel(
    nnz_ref, columns_ref, counts_ref, selected_ref, stats_ref, pca_ref,
    words, packed, scale_ref,
    gene_out, gene_in, pick_out, pick_in, dense_out, dense_in,
    x_out, x_in, xpick_out, xpick_in, y_out, y_in, ypick_out, ypick_in,
    send_gene, recv_gene, send_pick, recv_pick, send_dense, recv_dense,
    send_x, recv_x, send_y, recv_y,
):
    gx, gy, gz = lax.axis_index("gx"), lax.axis_index("gy"), lax.axis_index("gz")
    nx, ny, nz = lax.axis_size("gx"), lax.axis_size("gy"), lax.axis_size("gz")
    cells = 32 * nx * ny * nz

    barrier = pltpu.get_barrier_semaphore()

    def greet(axis, me, n):
        def one(d, carry):
            pl.semaphore_signal(
                barrier, inc=1, device_id={axis: lax.rem(me + d, n)}, device_id_type=MESH
            )
            return carry

        lax.fori_loop(1, n, one, 0)

    greet("gz", gz, nz)
    greet("gx", gx, nx)
    greet("gy", gy, ny)

    rows = iota((32, 1), 0)
    live = jnp.zeros((32, 1), i32)
    for c in range(32):
        live = jnp.where(rows == c, nnz_ref[c], live)
    tiles, library = [], jnp.zeros((32, 128), f32)
    for t in range(16):
        part = pl.ds(128 * t, 128)
        slot = iota((32, 128), 1) + 128 * t
        raw = jnp.where(slot < live, counts_ref[:, part], 0)
        library = library + raw.astype(f32)
        tiles.append(make_words(columns_ref[:, part], raw).astype(f32))
    scale = target_sum / jnp.sum(library, axis=1, keepdims=True)
    scale_ref[...] = jnp.broadcast_to(scale, (32, 128))
    for owner, tile in enumerate(sort_rows(tiles)):
        word = tile.astype(i32) & 1023
        words[owner] = word
        packed[owner] = (word[:16] << 10) | word[16:]

    pick = (iota((16, 256), 1) >> 4) == iota((16, 256), 0)
    pick = jnp.where(pick, f32(1.0), f32(0.0)).astype(bf16)

    def gene_sums(t, carry):
        word = words[t]
        value = jnp.log(1.0 + (word & 63).astype(f32) * scale_ref[...])
        low = (word >> 6).astype(f32).astype(bf16)
        terms = []
        for term in (value.astype(bf16), (value * value).astype(bf16)):
            folded = []
            for l in range(16):
                kept = jnp.where(low == bf16(l), term, bf16(0.0))
                folded.append(kept[:16] + kept[16:])
            terms.append(jnp.concatenate(folded, axis=0))
        terms = jnp.concatenate(terms, axis=1)
        sums = jnp.dot(pick, terms, preferred_element_type=f32)
        gene_out[t] = sums.astype(bf16)
        return carry

    lax.fori_loop(0, nz, gene_sums, 0)

    pl.semaphore_wait(barrier, (nx - 1) + (ny - 1) + (nz - 1))

    def to(axis, me, n, d, out, into, send, recv, whole=False):
        other = lax.rem(me + d, n)
        return pltpu.make_async_remote_copy(
            src_ref=out if whole else out.at[other],
            dst_ref=into.at[me],
            send_sem=send.at[other],
            recv_sem=recv.at[me],
            device_id={axis: other},
            device_id_type=MESH,
        )

    def came(axis, me, n, d, out, into, send, recv, whole=False):
        other = lax.rem(me + d, n)
        return pltpu.make_async_remote_copy(
            src_ref=out if whole else out.at[other],
            dst_ref=into.at[other],
            send_sem=send.at[other],
            recv_sem=recv.at[other],
            device_id={axis: other},
            device_id_type=MESH,
        )

    def start(*args, **kw):
        n = args[2]

        def one(d, carry):
            to(*args[:3], d, *args[3:], **kw).start()
            return carry

        lax.fori_loop(1, n, one, 0)

    def finish(*args, **kw):
        n = args[2]

        def one(d, carry):
            copy = came(*args[:3], d, *args[3:], **kw)
            copy.wait_recv()
            copy.wait_send()
            return carry

        lax.fori_loop(1, n, one, 0)

    z = ("gz", gz, nz)
    gene = z + (gene_out, gene_in, send_gene, recv_gene)
    picks = z + (pick_out, pick_in, send_pick, recv_pick)
    dense = z + (dense_out, dense_in, send_dense, recv_dense)
    start(*gene)

    def gather(k, carry):
        gene_id = selected_ref[pl.ds(k, 1), :]
        block = gene_id >> 4
        lane = jnp.broadcast_to(block & 127, (16, 128))
        tile = block >> 7
        got = jnp.zeros((16, 128), i32)
        for t in range(16):
            here = jnp.take_along_axis(packed[t], lane, axis=1, mode="promise_in_bounds")
            got = jnp.where(tile == t, here, got)
        word = jnp.concatenate([got >> 10, got & 1023], axis=0)
        count = jnp.where((word >> 6) == (gene_id & 15), word & 63, 0).astype(f32)
        value = jnp.log(1.0 + count * scale_ref[...])
        dense_out[k] = value.astype(bf16)
        pick_out[k] = jnp.concatenate(
            [jnp.sum(value, axis=0, keepdims=True), jnp.sum(value * value, axis=0, keepdims=True)],
            axis=0,
        )
        return carry

    lax.fori_loop(0, nz, gather, 0)
    start(*picks)
    start(*dense)
    gene_in[gz] = gene_out[gz]
    pick_in[gz] = pick_out[gz]
    dense_in[gz] = dense_out[gz]

    finish(*gene)
    finish(*picks)
    x_out[...] = jnp.sum(gene_in[...].astype(f32), axis=0)
    xpick_out[...] = jnp.sum(pick_in[...], axis=0)

    def add_over(axis, me, n, out, into, pick_out_, pick_in_, send, recv):
        a = (axis, me, n, out, into, send.at[0], recv.at[0])
        b = (axis, me, n, pick_out_, pick_in_, send.at[1], recv.at[1])
        start(*a, whole=True)
        start(*b, whole=True)
        into[me] = out[...]
        pick_in_[me] = pick_out_[...]
        finish(*a, whole=True)
        finish(*b, whole=True)
        return jnp.sum(into[...], axis=0), jnp.sum(pick_in_[...], axis=0)

    y_out[...], ypick_out[...] = add_over(
        "gx", gx, nx, x_out, x_in, xpick_out, xpick_in, send_x, recv_x
    )
    sums, picked = add_over("gy", gy, ny, y_out, y_in, ypick_out, ypick_in, send_y, recv_y)

    mean = sums[:, :128] / cells
    stats_ref[0] = mean
    stats_ref[1] = sums[:, 128:] / cells - mean * mean

    sel_mean = picked[0:1] / cells
    sel_variance = picked[1:2] / cells - sel_mean * sel_mean
    factor = 1.0 / jnp.sqrt(jnp.maximum(sel_variance, var_floor))
    finish(*dense)
    for s in range(16):
        value = (dense_in[s].astype(f32) - sel_mean) * factor
        pca_ref[32 * s : 32 * s + 32] = jnp.clip(value, -clip_value, clip_value).astype(bf16)


def per_device(columns, counts, nnz_count, selected):
    nz = lax.axis_size("gz")
    vmem = pl.BlockSpec(memory_space=pltpu.VMEM)
    dma = pltpu.SemaphoreType.DMA
    stats, pca = pl.pallas_call(
        kernel,
        out_shape=(
            jax.ShapeDtypeStruct((2, 16, 128), f32),
            jax.ShapeDtypeStruct((512, 128), bf16),
        ),
        in_specs=[pl.BlockSpec(memory_space=pltpu.SMEM), vmem, vmem, vmem],
        out_specs=(vmem, vmem),
        scratch_shapes=[
            pltpu.VMEM((16, 32, 128), i32),
            pltpu.VMEM((16, 16, 128), i32),
            pltpu.VMEM((32, 128), f32),
            pltpu.VMEM((16, 16, 256), bf16),
            pltpu.VMEM((16, 16, 256), bf16),
            pltpu.VMEM((16, 2, 128), f32),
            pltpu.VMEM((16, 2, 128), f32),
            pltpu.VMEM((16, 32, 128), bf16),
            pltpu.VMEM((16, 32, 128), bf16),
            pltpu.VMEM((16, 256), f32),
            pltpu.VMEM((4, 16, 256), f32),
            pltpu.VMEM((2, 128), f32),
            pltpu.VMEM((4, 2, 128), f32),
            pltpu.VMEM((16, 256), f32),
            pltpu.VMEM((4, 16, 256), f32),
            pltpu.VMEM((2, 128), f32),
            pltpu.VMEM((4, 2, 128), f32),
            dma((16,)), dma((16,)), dma((16,)), dma((16,)), dma((16,)), dma((16,)),
            dma((2, 4)), dma((2, 4)), dma((2, 4)), dma((2, 4)),
        ],
        compiler_params=pltpu.CompilerParams(collective_id=0, has_side_effects=True),
    )(nnz_count, columns, counts, selected.reshape(16, 128))
    return stats.transpose(0, 2, 1).reshape(2, 2048), pca


def solution(mesh):
    return jax.shard_map(
        per_device,
        mesh=mesh,
        in_specs=(
            P(("gx", "gy", "gz"), None),
            P(("gx", "gy", "gz"), None),
            P(("gx", "gy", "gz")),
            P(),
        ),
        out_specs=(P(None, "gz"), P(("gx", "gy"), "gz")),
        check_vma=False,
    )
```

```python
import jax
import jax.numpy as jnp
from jax import lax
from jax.experimental import pallas as pl
from jax.experimental.pallas import tpu as pltpu
from jax.sharding import PartitionSpec as P

target_sum = 10000.0
var_floor = 0.01
clip_value = 10.0
MESH = pl.DeviceIdType.MESH
f32, bf16, i32 = jnp.float32, jnp.bfloat16, jnp.int32


def iota(shape, dim):
    return lax.broadcasted_iota(i32, shape, dim)


def vreg_stage(x, j, p):
    n = x.shape[0]
    if p is None:
        y = x.reshape(n >> (j + 1), 2, 1 << j, 8, 128)
        a, b = y[:, 0], y[:, 1]
        out = jnp.stack([jnp.minimum(a, b), jnp.maximum(a, b)], axis=1)
    else:
        y = x.reshape(n >> (p + 1), 2, 1 << (p - j - 1), 2, 1 << j, 8, 128)
        a, b = y[:, :, :, 0], y[:, :, :, 1]
        lo, hi = jnp.minimum(a, b), jnp.maximum(a, b)
        first = jnp.stack([lo[:, 0], hi[:, 1]], axis=1)
        second = jnp.stack([hi[:, 0], lo[:, 1]], axis=1)
        out = jnp.stack([first, second], axis=3)
    return out.reshape(n, 8, 128)


def sublane_stage(x, d):
    rows = iota(x.shape, 1)
    other = jnp.take_along_axis(x, rows ^ d, axis=1, mode="promise_in_bounds")
    return jnp.where((rows & d) == 0, jnp.minimum(x, other), jnp.maximum(x, other))


def lane_stage(x, d):
    flat = x.reshape(x.shape[0] * 8, 128)
    lanes = iota(flat.shape, 1)
    other = jnp.take_along_axis(flat, lanes ^ d, axis=1, mode="promise_in_bounds")
    out = jnp.where((lanes & d) == 0, jnp.minimum(flat, other), jnp.maximum(flat, other))
    return out.reshape(x.shape)


def sort_words(x):
    place = iota((1, 8, 128), 1) * 64 + (iota((1, 8, 128), 2) >> 5) * 512

    def sign(p):
        return jnp.where(((place >> p) & 1) == 0, f32(1.0), f32(-1.0))

    held = None
    for p in range(1, 12):
        if p >= 6:
            change = sign(p) if p < 11 else None
            if held is not None:
                change = held if change is None else change * held
            x = x * change
            held = sign(p)
        for j in reversed(range(p)):
            if j >= 9:
                x = lane_stage(x, 32 << (j - 9))
            elif j >= 6:
                x = sublane_stage(x, 1 << (j - 6))
            else:
                x = vreg_stage(x, j, p if p < 6 else None)
    return x


def make_words(columns, raw):
    place = ((columns << 6) & ((0x600 << 10) | (15 << 6))) | ((columns << 12) & (7 << 16))
    return place | ((columns << 3) & (63 << 10)) | raw


def sort_rows(tiles):
    x = jnp.concatenate(
        [jnp.concatenate(tiles[4 * m : 4 * m + 4], axis=0).T for m in range(4)], axis=0
    )
    x = sort_words(x.reshape(64, 8, 128)).reshape(4, 128, 128)
    turned = [x[m].T for m in range(4)]
    return [turned[owner % 4][32 * (owner // 4) : 32 * (owner // 4) + 32] for owner in range(16)]


def in_gene_order(stat):
    lanes = (iota((16, 128), 1) & 15) * 8
    parts = [
        jnp.take_along_axis(stat, lanes + r, axis=1, mode="promise_in_bounds") for r in range(8)
    ]
    return jnp.concatenate(parts, axis=0).T[:16]


def kernel(
    nnz_ref, columns_ref, counts_ref, selected_ref, stats_ref, pca_ref,
    words, packed, scale_ref,
    gene_out, gene_in, pick_out, pick_in, dense_out, dense_in,
    x_out, x_in, xpick_out, xpick_in, y_out, y_in, ypick_out, ypick_in,
    send_gene, recv_gene, send_pick, recv_pick, send_dense, recv_dense,
    send_x, recv_x, send_y, recv_y,
):
    gx, gy, gz = lax.axis_index("gx"), lax.axis_index("gy"), lax.axis_index("gz")
    nx, ny, nz = lax.axis_size("gx"), lax.axis_size("gy"), lax.axis_size("gz")
    cells = 32 * nx * ny * nz

    barrier = pltpu.get_barrier_semaphore()

    def greet(axis, me, n):
        def one(d, carry):
            pl.semaphore_signal(
                barrier, inc=1, device_id={axis: lax.rem(me + d, n)}, device_id_type=MESH
            )
            return carry

        lax.fori_loop(1, n, one, 0)

    greet("gz", gz, nz)
    greet("gx", gx, nx)
    greet("gy", gy, ny)

    rows = iota((32, 1), 0)
    live = jnp.zeros((32, 1), i32)
    for c in range(32):
        live = jnp.where(rows == c, nnz_ref[c], live)
    tiles, library = [], jnp.zeros((32, 128), f32)
    for t in range(16):
        part = pl.ds(128 * t, 128)
        slot = iota((32, 128), 1) + 128 * t
        raw = jnp.where(slot < live, counts_ref[:, part], 0)
        library = library + raw.astype(f32)
        tiles.append(make_words(columns_ref[:, part], raw).astype(f32))
    scale = target_sum / jnp.sum(library, axis=1, keepdims=True)
    scale_ref[...] = jnp.broadcast_to(scale, (32, 128))
    for owner, tile in enumerate(sort_rows(tiles)):
        word = tile.astype(i32) & 1023
        words[owner] = word
        packed[owner] = (word[:16] << 10) | word[16:]

    pick = (iota((16, 256), 1) >> 4) == iota((16, 256), 0)
    pick = jnp.where(pick, f32(1.0), f32(0.0)).astype(bf16)

    def gene_sums(t):
        word = words[t]
        value = jnp.log(1.0 + (word & 63).astype(f32) * scale_ref[...])
        low = (word >> 6).astype(f32).astype(bf16)
        terms = []
        for term in (value.astype(bf16), (value * value).astype(bf16)):
            folded = []
            for l in range(16):
                kept = jnp.where(low == bf16(l), term, bf16(0.0))
                folded.append(kept[:16] + kept[16:])
            terms.append(jnp.concatenate(folded, axis=0))
        terms = jnp.concatenate(terms, axis=1)
        sums = jnp.dot(pick, terms, preferred_element_type=f32)
        gene_out[t] = sums.astype(bf16)

    for t in range(16):
        gene_sums(t)

    pl.semaphore_wait(barrier, (nx - 1) + (ny - 1) + (nz - 1))

    def to(axis, me, n, d, out, into, send, recv, whole=False):
        other = lax.rem(me + d, n)
        return pltpu.make_async_remote_copy(
            src_ref=out if whole else out.at[other],
            dst_ref=into.at[me],
            send_sem=send.at[other],
            recv_sem=recv.at[me],
            device_id={axis: other},
            device_id_type=MESH,
        )

    def came(axis, me, n, d, out, into, send, recv, whole=False):
        other = lax.rem(me + d, n)
        return pltpu.make_async_remote_copy(
            src_ref=out if whole else out.at[other],
            dst_ref=into.at[other],
            send_sem=send.at[other],
            recv_sem=recv.at[other],
            device_id={axis: other},
            device_id_type=MESH,
        )

    def start(*args, **kw):
        n = args[2]

        def one(d, carry):
            to(*args[:3], d, *args[3:], **kw).start()
            return carry

        lax.fori_loop(1, n, one, 0)

    def finish(*args, **kw):
        n = args[2]

        def one(d, carry):
            copy = came(*args[:3], d, *args[3:], **kw)
            copy.wait_recv()
            copy.wait_send()
            return carry

        lax.fori_loop(1, n, one, 0)

    z = ("gz", gz, nz)
    gene = z + (gene_out, gene_in, send_gene, recv_gene)
    picks = z + (pick_out, pick_in, send_pick, recv_pick)
    dense = z + (dense_out, dense_in, send_dense, recv_dense)
    start(*gene)

    def gather(k):
        gene_id = selected_ref[k : k + 1, :]
        block = gene_id >> 4
        lane = jnp.broadcast_to(block & 127, (16, 128))
        tile = block >> 7
        got = jnp.zeros((16, 128), i32)
        for t in range(16):
            here = jnp.take_along_axis(packed[t], lane, axis=1, mode="promise_in_bounds")
            got = jnp.where(tile == t, here, got)
        word = jnp.concatenate([got >> 10, got & 1023], axis=0)
        count = jnp.where((word >> 6) == (gene_id & 15), word & 63, 0).astype(f32)
        value = jnp.log(1.0 + count * scale_ref[...])
        dense_out[k] = value.astype(bf16)
        pick_out[k] = jnp.concatenate(
            [jnp.sum(value, axis=0, keepdims=True), jnp.sum(value * value, axis=0, keepdims=True)],
            axis=0,
        )

    for k in range(16):
        gather(k)
    start(*picks)
    start(*dense)
    gene_in[gz] = gene_out[gz]
    pick_in[gz] = pick_out[gz]
    dense_in[gz] = dense_out[gz]

    finish(*gene)
    finish(*picks)
    x_out[...] = jnp.sum(gene_in[...].astype(f32), axis=0)
    xpick_out[...] = jnp.sum(pick_in[...], axis=0)

    def add_over(axis, me, n, out, into, pick_out_, pick_in_, send, recv):
        a = (axis, me, n, out, into, send.at[0], recv.at[0])
        b = (axis, me, n, pick_out_, pick_in_, send.at[1], recv.at[1])
        start(*a, whole=True)
        start(*b, whole=True)
        into[me] = out[...]
        pick_in_[me] = pick_out_[...]
        finish(*a, whole=True)
        finish(*b, whole=True)
        return jnp.sum(into[...], axis=0), jnp.sum(pick_in_[...], axis=0)

    y_out[...], ypick_out[...] = add_over(
        "gx", gx, nx, x_out, x_in, xpick_out, xpick_in, send_x, recv_x
    )
    sums, picked = add_over("gy", gy, ny, y_out, y_in, ypick_out, ypick_in, send_y, recv_y)

    mean = sums[:, :128] / cells
    variance = sums[:, 128:] / cells - mean * mean
    for row, stat in enumerate((mean, variance)):
        flat = in_gene_order(stat)
        for u in range(16):
            stats_ref[row : row + 1, 128 * u : 128 * u + 128] = flat[u : u + 1]

    sel_mean = picked[0:1] / cells
    sel_variance = picked[1:2] / cells - sel_mean * sel_mean
    factor = 1.0 / jnp.sqrt(jnp.maximum(sel_variance, var_floor))
    finish(*dense)
    for s in range(16):
        value = (dense_in[s].astype(f32) - sel_mean) * factor
        pca_ref[32 * s : 32 * s + 32] = jnp.clip(value, -clip_value, clip_value).astype(bf16)


def per_device(columns, counts, nnz_count, selected):
    nz = lax.axis_size("gz")
    vmem = pl.BlockSpec(memory_space=pltpu.VMEM)
    dma = pltpu.SemaphoreType.DMA
    stats, pca = pl.pallas_call(
        kernel,
        out_shape=(
            pltpu.VMEM((2, 2048), f32),
            pltpu.VMEM((512, 128), bf16),
        ),
        in_specs=[pl.BlockSpec(memory_space=pltpu.SMEM), vmem, vmem, vmem],
        out_specs=(vmem, vmem),
        scratch_shapes=[
            pltpu.VMEM((16, 32, 128), i32),
            pltpu.VMEM((16, 16, 128), i32),
            pltpu.VMEM((32, 128), f32),
            pltpu.VMEM((16, 16, 256), bf16),
            pltpu.VMEM((16, 16, 256), bf16),
            pltpu.VMEM((16, 2, 128), f32),
            pltpu.VMEM((16, 2, 128), f32),
            pltpu.VMEM((16, 32, 128), bf16),
            pltpu.VMEM((16, 32, 128), bf16),
            pltpu.VMEM((16, 256), f32),
            pltpu.VMEM((4, 16, 256), f32),
            pltpu.VMEM((2, 128), f32),
            pltpu.VMEM((4, 2, 128), f32),
            pltpu.VMEM((16, 256), f32),
            pltpu.VMEM((4, 16, 256), f32),
            pltpu.VMEM((2, 128), f32),
            pltpu.VMEM((4, 2, 128), f32),
            dma((16,)), dma((16,)), dma((16,)), dma((16,)), dma((16,)), dma((16,)),
            dma((2, 4)), dma((2, 4)), dma((2, 4)), dma((2, 4)),
        ],
        compiler_params=pltpu.CompilerParams(collective_id=0, has_side_effects=True),
    )(nnz_count, columns, counts, selected.reshape(16, 128))
    return stats, pca


def solution(mesh):
    return jax.shard_map(
        per_device,
        mesh=mesh,
        in_specs=(
            P(("gx", "gy", "gz"), None),
            P(("gx", "gy", "gz"), None),
            P(("gx", "gy", "gz")),
            P(),
        ),
        out_specs=(P(None, "gz"), P(("gx", "gy"), "gz")),
        check_vma=False,
    )
```
